32 devices in a mesh: expert: 2 (over x), tensor: 16 (over z, y, core).
Axes of the slice: x: 2, y: 2, z: 4, core: 2. Of those that a mesh axis runs over, the one named last changes fastest.
Arguments:
- tokens: bfloat16 [96, 6144], P('expert', 'tensor'), may hold values from -6 to 6
- expert_ids: int32 [96, 2], P('expert'), may hold values from 0 to 1, as said below
- route_weight: int32 [96, 2], P('expert'), may hold values from 1 to 4095
- gate_weight: bfloat16 [2, 6144, 8192], P('expert', None, 'tensor'), may hold values from -0.078125 to 0.078125
- up_weight: bfloat16 [2, 6144, 8192], P('expert', None, 'tensor'), may hold values from -0.078125 to 0.078125
- down_weight: bfloat16 [2, 8192, 6144], P('expert', 'tensor'), may hold values from -0.0625 to 0.0625
Outputs:
- mixed: bfloat16 [96, 6144], P('expert', 'tensor')
- expert_load: float32 [2, 2], replicated
The draws below stay inside these ranges and needn't reach their ends.
Inputs may be any that keep to these rules, and one draw needn't show every extreme that they name: `expert_ids`: each row names two different experts. The hot expert is the one named in the first column of the first row of every aligned block of 48 rows (the tokens of one expert group), the same in all blocks. In each block exactly 48 rows name the hot expert, in either column; every other expert is named by 7 or 48 rows of each block, and by exactly 48 rows in some.
All inputs are finite; a program needn't handle non-finite values.
Results may differ from the reference program's by a relative error of at most 0.005.
Values may be sent and summed in bfloat16 or wider, within the bound.
A program may use at most 64 MiB of HBM per device.

```python
import jax
import jax.numpy as jnp
from jax import lax

D = 6144
FF = 8192
TOK_DEV = 48
EXPERTS = 2
TOKENS = 96
HOT_ROWS = 48
CAP = 48


def draw_expert_ids(key, part):
    hot_id = jax.random.randint(jax.random.fold_in(key, 101), (1,), 0, EXPERTS).astype(jnp.int32)[0]
    block_count = TOKENS // TOK_DEV
    cold_count = EXPERTS - 1
    scores = jax.random.randint(jax.random.fold_in(key, 202), (block_count, TOK_DEV), 0, 1048576).astype(jnp.int32)
    scores = scores * TOK_DEV + jnp.arange(TOK_DEV, dtype=jnp.int32)[None, :]
    scores = jnp.where(jnp.arange(TOK_DEV, dtype=jnp.int32)[None, :] == 0, jnp.int32(-1), scores)
    order = jnp.argsort(scores, axis=1, stable=True).astype(jnp.int32)
    rank = jnp.argsort(order, axis=1, stable=True).astype(jnp.int32)
    rotation = jax.random.randint(jax.random.fold_in(key, 303), (block_count, 1), 0, cold_count).astype(jnp.int32)
    first_slot = jnp.where(rank < HOT_ROWS, rank, HOT_ROWS + 2 * (rank - HOT_ROWS))
    second_slot = jnp.where(rank < HOT_ROWS, rank, first_slot + 1)

    def cold_label(slot_number):
        shifted = (slot_number + rotation) % cold_count
        return shifted + (shifted >= hot_id).astype(jnp.int32)
    first = jnp.where(rank < HOT_ROWS, hot_id, cold_label(first_slot))
    second = cold_label(second_slot)
    flips = jax.random.randint(jax.random.fold_in(key, 404), (block_count, TOK_DEV), 0, 2).astype(jnp.int32)
    flips = jnp.where(jnp.arange(TOK_DEV, dtype=jnp.int32)[None, :] == 0, jnp.int32(0), flips)
    left = jnp.where(flips == 1, second, first)
    right = jnp.where(flips == 1, first, second)
    return jnp.stack([left, right], axis=2).reshape(TOKENS, 2).astype(jnp.int32)


def place_ends(array, key, low, top_value):
    spot = [jax.random.randint(jax.random.fold_in(key, axis), (), 0, length) for axis, length in enumerate(array.shape)]
    longest = array.shape.index(max(array.shape))
    neighbour = spot[:longest] + [(spot[longest] + 1) % array.shape[longest]] + spot[longest + 1:]
    return array.at[tuple(spot)].set(low).at[tuple(neighbour)].set(top_value)


def levels(key, shape, split, smallest, high):
    loudness = 1.0
    for position, parts in split:
        steps = jax.random.uniform(jax.random.fold_in(jax.random.fold_in(key, 6), position), (parts,), jnp.float32, smallest / len(split), high / len(split))
        loudness = loudness * jnp.repeat(jnp.exp(steps), shape[position] // parts).reshape((-1,) + (1,) * (len(shape) - 1 - position))
    return loudness


def centred(own_key, shape, deviation, reach, pieces=(), held_as=jnp.bfloat16):
    values = jax.random.normal(own_key, shape, jnp.float32) * deviation
    if len(pieces) > 0:
        values = levels(own_key, shape, pieces, -0.22, 0.18) * values
    return jnp.clip(values, min=-reach, max=reach).astype(held_as)


def setup_inputs(seed: int = 0) -> dict:
    streams_of = jax.random.split(jax.random.key(seed), 7)
    return {
        "tokens": centred(streams_of[0], (TOKENS, D), 1.0, 6.0, ((0, 2), (1, 16))),
        "expert_ids": draw_expert_ids(jax.random.fold_in(streams_of[6], 71), 0),
        "route_weight": place_ends(jax.random.randint(streams_of[2], (TOKENS, 2), 1, 4096), jax.random.fold_in(streams_of[2], 1), 1, 4095).astype(jnp.int32),
        "gate_weight": centred(streams_of[3], (EXPERTS, D, FF), D ** -0.5, 0.078125, ((0, 2), (2, 16))),
        "up_weight": centred(streams_of[4], (EXPERTS, D, FF), D ** -0.5, 0.078125, ((0, 2), (2, 16))),
        "down_weight": centred(streams_of[5], (EXPERTS, FF, D), FF ** -0.5, 0.0625, ((0, 2), (1, 16))),
    }


def expert_ffn(row_block, w_gate, w_up, w_down):
    gate_value = jnp.dot(row_block, w_gate, preferred_element_type=jnp.float32)
    up_value = jnp.dot(row_block, w_up, preferred_element_type=jnp.float32)
    hidden = (jax.nn.silu(gate_value) * up_value).astype(jnp.bfloat16)
    return jnp.dot(hidden, w_down, preferred_element_type=jnp.float32)


def reference(tokens, expert_ids, route_weight, gate_weight, up_weight, down_weight):
    weights = route_weight.astype(jnp.float32)
    route_share = weights / jnp.sum(weights, axis=1, keepdims=True)
    labels = jnp.arange(EXPERTS, dtype=jnp.int32)
    chosen = expert_ids[:, :, None] == labels[None, None, :]
    mixing = jnp.sum(jnp.where(chosen, route_share[:, :, None], jnp.float32(0.0)), axis=1)
    hot_id = expert_ids[0, 0]

    def add_rows(running, row_mask, most_rows, expert):
        row_index = jnp.nonzero(row_mask, size=most_rows, fill_value=0)[0].astype(jnp.int32)
        counted = jnp.sum(row_mask.astype(jnp.int32))
        is_valid = jnp.arange(most_rows, dtype=jnp.int32) < counted
        expert_out = expert_ffn(tokens[row_index], gate_weight[expert], up_weight[expert], down_weight[expert])
        row_scale = jnp.where(is_valid, mixing[row_index, expert], jnp.float32(0.0))
        return running.at[row_index].add(row_scale[:, None] * expert_out)

    running = jnp.zeros((TOKENS, D), jnp.float32)
    hot_mask = jnp.any(expert_ids == hot_id, axis=1)
    running = add_rows(running, hot_mask, EXPERTS * HOT_ROWS, hot_id)

    def cold_step(carry, expert):
        cold_mask = jnp.any(expert_ids == expert, axis=1) & (expert != hot_id)
        return add_rows(carry, cold_mask, EXPERTS * CAP, expert), None

    running, unused = lax.scan(cold_step, running, labels)
    counts = jnp.sum(chosen.astype(jnp.float32), axis=(0, 1))
    expert_load = jnp.stack([counts, jnp.sum(mixing, axis=0)]) / TOK_DEV
    return running.astype(jnp.bfloat16), expert_load
```

```python
import functools

import jax
import jax.numpy as jnp
from jax import lax
from jax.experimental import pallas as pl
from jax.experimental.pallas import tpu as pltpu
from jax.sharding import PartitionSpec as P

MESH = pl.DeviceIdType.MESH
LANES = 128


def near_first(step, count):
    return ((step + 1) // 2) * (2 * (step % 2) - 1) + count


def kernel(
    depth,
    tok_ref, ids_ref, raw_ref, gate_hbm, up_hbm, down_hbm,
    out_ref, load_ref,
    tok_all, gate_buf, up_buf, down_buf, gate_acc, up_acc, hidden,
    keep, pair_out, pair_in, rs_out, in_one, out_two, in_two, out_three, in_three,
    ids_in, raw_in, mix,
    gate_sem, up_sem, down_sem, own_sem,
    z_send, one_send, two_send, sib_send, ag_recv,
    pair_send, pair_recv, rs_one_send, rs_one_recv, rs_two_send, rs_two_recv, rs_z_send, rs_z_recv,
    st_send, st_recv,
):
    rows, width = tok_ref.shape
    wide = 2 * width
    e = lax.axis_index("expert")
    t = lax.axis_index("tensor")
    c = t % 2
    y = (t // 2) % 2
    z = t // 4
    e_one, y_one = e + (1 - c) * (1 - 2 * e), y + c * (1 - 2 * y)
    e_two, y_two = e + c * (1 - 2 * e), y + (1 - c) * (1 - 2 * y)
    lines = ((e, y), (e_one, y_one), (e_two, y_two), (1 - e, 1 - y))

    def device(e2, z2, y2, c2):
        return (e2, 4 * z2 + 2 * y2 + c2)

    first = device(e_one, z, y_one, c)
    second = device(e_two, z, y_two, c)
    sibling = device(e, z, y, 1 - c)
    across = device(1 - e, z, y, c)

    def z_at(step):
        return (z + near_first(step, depth)) % depth

    def chip(z2, y2):
        return 2 * z2 + y2

    def row_span(e2):
        return pl.ds(pl.multiple_of(e2 * rows, 16), rows)

    def weight_copies(m):
        span = pl.ds(pl.multiple_of(m * wide, LANES), wide)
        return (
            pltpu.make_async_copy(gate_hbm.at[0, span, :], gate_buf.at[m], gate_sem.at[m]),
            pltpu.make_async_copy(up_hbm.at[0, span, :], up_buf.at[m], up_sem.at[m]),
        )

    def down_copy(m):
        span = pl.ds(pl.multiple_of(m * wide, LANES), wide)
        return pltpu.make_async_copy(down_hbm.at[0, :, span], down_buf.at[m], down_sem.at[m])

    def slot(e2, z2, y2, parity):
        lanes = pl.ds(pl.multiple_of(parity * width, LANES), width)
        return tok_all.at[chip(z2, y2), row_span(e2), lanes]

    for y2 in (y, 1 - y):
        for step in range(depth):
            for copy in weight_copies(chip(z_at(step), y2)):
                copy.start()
    for step in range(depth):
        for y2 in (1 - y, y):
            down_copy(chip(z_at(depth - 1 - step), y2)).start()

    own_copy = pltpu.make_async_copy(tok_ref, slot(e, z, y, c), own_sem)
    own_copy.start()

    barrier = pltpu.get_barrier_semaphore()
    friends = [sibling, first, second]
    friends += [device(e, z_at(step), y, c) for step in range(1, depth)]
    for friend in friends:
        pl.semaphore_signal(barrier, inc=1, device_id=friend, device_id_type=MESH)
    pl.semaphore_wait(barrier, len(friends))

    def remote(src, dst, send, recv, target):
        return pltpu.make_async_remote_copy(
            src_ref=src, dst_ref=dst, send_sem=send, recv_sem=recv,
            device_id=target, device_id_type=MESH,
        )

    def token_copy(source, e2, z2, y2, send, target):
        place = slot(e2, z2, y2, c)
        arrived = ag_recv.at[e2, 4 * z2 + 2 * y2 + c]
        return remote(place if source is None else source, place, send, arrived, target)

    def spread(line, step, source=None):
        e2, y2 = lines[line]
        z2 = z_at(step)
        copies = []
        if line == 0:
            copies.append(token_copy(source, e2, z2, y2, one_send.at[step], first))
        if line <= 1:
            copies.append(token_copy(source, e2, z2, y2, two_send.at[line, step], second))
        copies.append(token_copy(source, e2, z2, y2, sib_send.at[line, step], sibling))
        return copies

    def z_copy(step):
        return token_copy(tok_ref, e, z, y, z_send.at[step], device(e, z_at(step), y, c))

    def token_wait(e2, z2, y2, parity):
        place = slot(e2, z2, y2, parity)
        remote(place, place, own_sem, ag_recv.at[e2, 4 * z2 + 2 * y2 + parity], sibling).wait_recv()

    def stat_copies():
        return (
            remote(ids_ref, ids_in, st_send.at[0], st_recv.at[0], across),
            remote(raw_ref, raw_in, st_send.at[1], st_recv.at[1], across),
        )

    for step in range(1, depth):
        z_copy(step).start()
    for copy in spread(0, 0, tok_ref):
        copy.start()
    for copy in stat_copies():
        copy.start()

    gate_acc[...] = jnp.zeros_like(gate_acc)
    up_acc[...] = jnp.zeros_like(up_acc)
    own_copy.wait()

    for line in range(3):
        for step in range(depth):
            if (line, step) == (0, 0):
                continue
            e2, y2 = lines[line]
            token_wait(e2, z_at(step), y2, c)
            for copy in spread(line, step):
                copy.start()

    for copy in stat_copies():
        copy.wait_recv()
    held = []
    for ids_part, raw_part in ((ids_ref, raw_ref), (ids_in, raw_in)):
        ids = ids_part[...]
        raw = raw_part[...].astype(jnp.float32)
        held.append((ids, raw / jnp.sum(raw, axis=0, keepdims=True)))
    square = (rows, rows)
    diagonal = lax.broadcasted_iota(jnp.int32, square, 0) == lax.broadcasted_iota(jnp.int32, square, 1)
    for (ids, share), e2 in zip(held, (e, 1 - e)):
        line_mix = jnp.sum(jnp.where(ids == e, share, 0.0), axis=0, keepdims=True)
        column = jnp.sum(jnp.where(diagonal, line_mix, 0.0), axis=1, keepdims=True)
        mix[row_span(e2), :] = jnp.broadcast_to(column, (rows, LANES))
    row_at = lax.broadcasted_iota(jnp.int32, (2, 2), 0)
    lane_at = lax.broadcasted_iota(jnp.int32, (2, 2), 1)
    load = jnp.zeros((2, 2), jnp.float32)
    for label in range(2):
        counts, weights = [], []
        for ids, share in held:
            hit = ids == label
            counts.append(jnp.sum(hit.astype(jnp.float32), axis=(0, 1), keepdims=True))
            weights.append(jnp.sum(jnp.where(hit, share, 0.0), axis=(0, 1), keepdims=True))
        load = jnp.where((lane_at == label) & (row_at == 0), counts[0] + counts[1], load)
        load = jnp.where((lane_at == label) & (row_at == 1), weights[0] + weights[1], load)
    load_ref[...] = load / rows

    def first_layer(m):
        for copy in weight_copies(m):
            copy.wait()
        left = tok_all[m]
        gate_acc[...] += jnp.dot(left, gate_buf[m], preferred_element_type=jnp.float32)
        up_acc[...] += jnp.dot(left, up_buf[m], preferred_element_type=jnp.float32)

    def last_blocks(step):
        e2, y2 = lines[3]
        token_wait(e2, z_at(step), y2, c)
        for copy in spread(3, step):
            copy.start()

    @pl.loop(0, depth)
    def _(step):
        last_blocks(step)
        for e2 in (e, 1 - e):
            token_wait(e2, z_at(step), y, 1 - c)
        first_layer(chip(z_at(step), y))

    @pl.loop(0, depth)
    def _(step):
        for e2 in (e, 1 - e):
            token_wait(e2, z_at(step), 1 - y, 1 - c)
        first_layer(chip(z_at(step), 1 - y))

    gate = gate_acc[...]
    hidden[...] = (gate / (1.0 + jnp.exp(-gate)) * up_acc[...]).astype(hidden.dtype)

    def pair_copy(m):
        return remote(pair_out.at[m], pair_in.at[m], pair_send.at[m], pair_recv.at[m], sibling)

    def send_one(line, z2):
        e2, y2 = lines[line]
        return remote(
            rs_out.at[chip(z2, y2), row_span(e2)], in_one.at[line - 2, z2],
            rs_one_send.at[line - 2, z2], rs_one_recv.at[line - 2, z2], second,
        )

    def send_two(z2):
        return remote(out_two.at[z2], in_two.at[z2], rs_two_send.at[z2], rs_two_recv.at[z2], first)

    def send_three(z2):
        target = device(e, z2, y, c)
        return remote(out_three.at[z2], in_three.at[z], rs_z_send.at[z2], rs_z_recv.at[z], target)

    def second_layer(m):
        down_copy(m).wait()
        part = jnp.dot(hidden[...], down_buf[m], preferred_element_type=jnp.float32)
        part = part * mix[:, :1]
        low, high = part[:, :width], part[:, width:]
        pair_out[m] = jnp.where(c == 0, high, low).astype(pair_out.dtype)
        keep[m] = jnp.where(c == 0, low, high)
        pair_copy(m).start()

    def join_pair(z2):
        for y2 in (1 - y, y):
            m = chip(z2, y2)
            pair_copy(m).wait_recv()
            total = keep[m] + pair_in[m].astype(jnp.float32)
            keep[m] = total
            rs_out[m] = total.astype(rs_out.dtype)
        send_one(3, z2).start()
        send_one(2, z2).start()

    def far(step):
        return z_at(depth - 1 - step)

    for y2 in (1 - y, y):
        second_layer(chip(far(0), y2))

    @pl.loop(1, depth)
    def _(step):
        for y2 in (1 - y, y):
            second_layer(chip(far(step), y2))
        join_pair(far(step - 1))

    join_pair(far(depth - 1))

    for step in range(depth):
        z2 = far(step)
        send_one(3, z2).wait_recv()
        total = keep[chip(z2, y_one), row_span(e_one)] + in_one[1, z2].astype(jnp.float32)
        out_two[z2] = total.astype(out_two.dtype)
        send_two(z2).start()
    for step in range(depth):
        z2 = far(step)
        send_one(2, z2).wait_recv()
        send_two(z2).wait_recv()
        total = keep[chip(z2, y), row_span(e)] + in_one[0, z2].astype(jnp.float32)
        total += in_two[z2].astype(jnp.float32)
        if step < depth - 1:
            out_three[z2] = total.astype(out_three.dtype)
            send_three(z2).start()
    for step in range(1, depth):
        z2 = z_at(step)
        remote(in_three.at[z2], in_three.at[z2], own_sem, rs_z_recv.at[z2], sibling).wait_recv()
        total += in_three[z2].astype(jnp.float32)
    out_ref[...] = total.astype(out_ref.dtype)

    for step in range(depth):
        if step > 0:
            z_copy(step).wait_send()
            send_three(z_at(step)).wait_send()
        for line in range(4):
            for copy in spread(line, step):
                copy.wait_send()
        for y2 in (y, 1 - y):
            pair_copy(chip(z_at(step), y2)).wait_send()
        send_one(2, z_at(step)).wait_send()
        send_one(3, z_at(step)).wait_send()
        send_two(z_at(step)).wait_send()
    for copy in stat_copies():
        copy.wait_send()


def put_out(mixed_ref, load_ref, mixed_out, load_out, sems):
    copies = (
        pltpu.make_async_copy(mixed_ref, mixed_out, sems.at[0]),
        pltpu.make_async_copy(load_ref, load_out, sems.at[1]),
    )
    for copy in copies:
        copy.start()
    for copy in copies:
        copy.wait()


def fused(tokens, expert_ids, route_weight, gate_weight, up_weight, down_weight):
    groups, peers = lax.axis_size("expert"), lax.axis_size("tensor")
    rows, width = tokens.shape
    units = gate_weight.shape[2]
    depth, chips, wide, all_rows = peers // 4, peers // 2, 2 * width, groups * rows
    vmem = pl.BlockSpec(memory_space=pltpu.VMEM)
    anywhere = pl.BlockSpec(memory_space=pl.ANY)
    half, single, dma = jnp.bfloat16, jnp.float32, pltpu.SemaphoreType.DMA
    held = pl.pallas_call(
        functools.partial(kernel, depth),
        out_shape=(
            pltpu.VMEM((rows, width), half),
            pltpu.VMEM((2, groups), single),
        ),
        in_specs=[vmem, vmem, vmem, anywhere, anywhere, anywhere],
        out_specs=(vmem, vmem),
        scratch_shapes=[
            pltpu.VMEM((chips, all_rows, wide), half),
            pltpu.VMEM((chips, wide, units), half),
            pltpu.VMEM((chips, wide, units), half),
            pltpu.VMEM((chips, units, wide), half),
            pltpu.VMEM((all_rows, units), single),
            pltpu.VMEM((all_rows, units), single),
            pltpu.VMEM((all_rows, units), half),
            pltpu.VMEM((chips, all_rows, width), single),
            pltpu.VMEM((chips, all_rows, width), half),
            pltpu.VMEM((chips, all_rows, width), half),
            pltpu.VMEM((chips, all_rows, width), half),
            pltpu.VMEM((2, depth, rows, width), half),
            pltpu.VMEM((depth, rows, width), half),
            pltpu.VMEM((depth, rows, width), half),
            pltpu.VMEM((depth, rows, width), half),
            pltpu.VMEM((depth, rows, width), half),
            pltpu.VMEM((2, rows), jnp.int32),
            pltpu.VMEM((2, rows), jnp.int32),
            pltpu.VMEM((all_rows, LANES), single),
            dma((chips,)), dma((chips,)), dma((chips,)), dma(()),
            dma((depth,)), dma((depth,)), dma((2, depth)), dma((4, depth)), dma((groups, peers)),
            dma((chips,)), dma((chips,)), dma((2, depth)), dma((2, depth)),
            dma((depth,)), dma((depth,)), dma((depth,)), dma((depth,)),
            dma((2,)), dma((2,)),
        ],
        compiler_params=pltpu.CompilerParams(
            collective_id=0, has_side_effects=True, vmem_limit_bytes=60 * 1024 * 1024
        ),
    )(tokens, expert_ids.T, route_weight.T, gate_weight, up_weight, down_weight)
    held = [pltpu.with_memory_space_constraint(part, pltpu.VMEM) for part in held]
    return pl.pallas_call(
        put_out,
        out_shape=(
            jax.ShapeDtypeStruct((rows, width), half),
            jax.ShapeDtypeStruct((2, groups), single),
        ),
        in_specs=[vmem, vmem],
        out_specs=(pl.BlockSpec(memory_space=pltpu.HBM),) * 2,
        scratch_shapes=[dma((2,))],
    )(*held)


def fits(mesh, tokens):
    groups, peers = mesh.shape["expert"], mesh.shape["tensor"]
    rows, width = tokens.shape[0] // groups, tokens.shape[1] // peers
    return groups == 2 and peers % 4 == 0 and rows % 16 == 0 and width % LANES == 0


def swiglu(gate_value, up_value):
    return (jax.nn.silu(gate_value) * up_value).astype(jnp.bfloat16)


def matmul(left, right):
    return jnp.dot(left, right, preferred_element_type=jnp.float32)


def route_stats(id_block, raw_block, labels):
    weights = raw_block.astype(jnp.float32)
    route_share = weights / jnp.sum(weights, axis=1, keepdims=True)
    flat_chosen = (
        (id_block[:, :, None] == labels[None, None, :])
        .astype(jnp.int32)
        .reshape(-1, labels.shape[0])
    )
    chosen_float = flat_chosen.astype(jnp.float32)
    stats = jnp.stack(
        [jnp.sum(chosen_float, axis=0), jnp.sum(route_share.reshape(-1, 1) * chosen_float, axis=0)]
    )
    return (route_share, flat_chosen, stats)


def hot_inputs(hot_local, hot_id, labels):
    is_target = (labels == hot_id)[:, None, None]
    send_rows = jnp.where(is_target, hot_local[None], jnp.zeros_like(hot_local)[None])
    arrived = lax.all_to_all(send_rows, "expert", split_axis=0, concat_axis=0, tiled=True)
    return arrived.reshape(-1, hot_local.shape[1])


def local(tokens, expert_ids, route_weight, gate_weight, up_weight, down_weight):
    tok_rows = expert_ids.shape[0]
    experts = lax.axis_size("expert") * gate_weight.shape[0]
    hot_rows = tok_rows - tok_rows // 8 * min(experts - 2, 1)
    capacity = (2 * tok_rows - hot_rows + experts - 2) // (experts - 1)
    hot_id = expert_ids[0, 0]
    own_gate = gate_weight[0]
    own_up = up_weight[0]
    own_down = down_weight[0]
    hot_gate_w, hot_up_w, hot_down_w = (own_gate, own_up, own_down)
    labels = jnp.arange(experts, dtype=jnp.int32)
    route_share, flat_chosen, local_stats = route_stats(expert_ids, route_weight, labels)
    cold_chosen = flat_chosen * (labels != hot_id).astype(jnp.int32)[None, :]
    slot_index = jnp.sum((jnp.cumsum(cold_chosen, axis=0) - 1) * cold_chosen, axis=1)
    is_live = jnp.sum(cold_chosen, axis=1)
    target = jnp.sum(cold_chosen * labels[None, :], axis=1) * capacity + slot_index
    buffer_rows = jnp.arange(experts * capacity, dtype=jnp.int32)
    cold_pick = ((target[None, :] == buffer_rows[:, None]) & (is_live[None, :] == 1)).astype(
        jnp.bfloat16
    )
    cold_pick = jnp.sum(cold_pick.reshape(experts * capacity, tok_rows, 2), axis=2)
    hot_match = (expert_ids == hot_id).astype(jnp.int32)
    hot_flag = jnp.sum(hot_match, axis=1)
    hot_rank = jnp.cumsum(hot_flag) - 1
    hot_slots = jnp.arange(hot_rows, dtype=jnp.int32)
    hot_pick = ((hot_rank[None, :] == hot_slots[:, None]) & (hot_flag[None, :] == 1)).astype(
        jnp.bfloat16
    )
    feature_width = tokens.shape[1]
    cold_send = (
        matmul(cold_pick, tokens).astype(jnp.bfloat16).reshape(experts, capacity, feature_width)
    )
    cold_recv = lax.all_to_all(
        cold_send, "expert", split_axis=0, concat_axis=0, tiled=True
    ).reshape(experts * capacity, feature_width)
    hot_input = hot_inputs(matmul(hot_pick, tokens).astype(jnp.bfloat16), hot_id, labels)
    cold_piece = lax.all_gather(cold_recv, "tensor", axis=1, tiled=True)
    hot_piece = lax.all_gather(hot_input, "tensor", axis=1, tiled=True)
    cold_gate = matmul(cold_piece, own_gate)
    cold_up = matmul(cold_piece, own_up)
    hot_gate = matmul(hot_piece, hot_gate_w)
    hot_up = matmul(hot_piece, hot_up_w)
    cold_part = matmul(swiglu(cold_gate, cold_up), own_down)
    hot_part = matmul(swiglu(hot_gate, hot_up), hot_down_w)
    model_width = cold_part.shape[1]
    came_back = lax.all_to_all(
        hot_part.reshape(experts, hot_rows, model_width),
        "expert",
        split_axis=0,
        concat_axis=0,
        tiled=True,
    )
    hot_part = lax.dynamic_index_in_dim(came_back, hot_id, 0, keepdims=False)
    returned = lax.all_to_all(
        cold_part.reshape(experts, capacity, model_width),
        "expert",
        split_axis=0,
        concat_axis=0,
        tiled=True,
    ).reshape(experts * capacity, model_width)
    assign_weight = route_share.reshape(2 * tok_rows) * is_live.astype(jnp.float32)
    cold_out = jnp.sum(
        (returned[target] * assign_weight[:, None]).reshape(tok_rows, 2, model_width), axis=1
    )
    hot_weight = jnp.sum(route_share * hot_match.astype(jnp.float32), axis=1)
    hot_out = hot_part[jnp.clip(hot_rank, 0, hot_rows - 1)] * hot_weight[:, None]
    mixed = lax.psum_scatter(cold_out + hot_out, "tensor", scatter_dimension=1, tiled=True).astype(
        jnp.bfloat16
    )
    expert_load = lax.psum(local_stats, "expert") / tok_rows
    return (mixed, expert_load)


def solution(mesh):
    placed = (
        P("expert", "tensor"),
        P("expert", None),
        P("expert", None),
        P("expert", None, "tensor"),
        P("expert", None, "tensor"),
        P("expert", "tensor", None),
    )

    def run(tokens, *rest):
        body = fused if fits(mesh, tokens) else local
        return jax.shard_map(
            body,
            mesh=mesh,
            in_specs=placed,
            out_specs=(P("expert", "tensor"), P()),
            check_vma=False,
        )(tokens, *rest)

    return run
```
